32 devices in a mesh: rows: 8 (over y, x, core), cols: 4 (over z).
Axes of the slice: x: 2, y: 2, z: 4, core: 2. Of those that a mesh axis runs over, the one named last changes fastest.
Arguments:
- intensity: float32 [4096, 4096], P('rows', 'cols'), may hold values from -0.5 to 1.5, as said below
- edge_weight: float32 [4096, 4096], P('rows', 'cols'), may hold values from 0.2 to 2
- labels: int32 [4096, 4096], P('rows', 'cols'), may hold values from 0 to 1
- tile_cost: int32 [16, 16], replicated, may hold values from 0 to 3, as said below
- tile_owner: int32 [16, 16], replicated, may hold values from -1 to 31, as said below
Outputs:
- slot_field: float32 [32, 4, 256, 256], P('rows', 'cols')
The draws below stay inside these ranges and needn't reach their ends.
Inputs may be any that keep to these rules, and one draw needn't show every extreme that they name: `intensity`: intensity of stained tissue. `tile_cost`: 0 marks a background tile, 1 to 3 a tissue tile. `tile_owner`: -1 exactly for background tiles. A tissue tile's value is k * 4 + s: it goes to slot s of the device with rows index k in its own column band; within one band no two tiles share a value; the tiles of one device's block send at most 1 tile to any one device, and in every draw some block sends exactly 1 to one device and some device receives all 4 of its slots filled.
All inputs are finite; a program needn't handle non-finite values.
Results may differ from the reference program's by a relative error of at most 0.0001.
Values sent between devices are 32-bit elements; how exact they have to be, the bound alone decides.
A program may use at most 128 MiB of HBM per device.

```python
import math
import jax
import jax.numpy as jnp

TILE = 256
BLOCK_ROWS = 512
BLOCK_COLS = 1024
ITERS_BEFORE = 2
ITERS_AFTER = 2
TILE_SLOTS = 4
ROWS = 4096
COLS = 4096
TILE_ROWS = 16
TILE_COLS = 16
N_ROWS = 8
N_COLS = 4


def tissue_plan(key):
    base_key = jax.random.fold_in(key, 4242)
    key_count, key_pick, key_start, key_level = jax.random.split(base_key, 4)
    per_row = BLOCK_COLS // TILE
    stripes = COLS // BLOCK_COLS
    devices = ROWS // BLOCK_ROWS
    stripe_total = TILE_ROWS * per_row
    half_count = stripe_total // 2
    low_count = 3 * stripe_total // 8
    counts = jax.random.randint(key_count, (stripes,), low_count, half_count + 1)
    forced = jax.random.randint(key_pick, (), 0, stripes)
    counts = jnp.where(jnp.arange(stripes) == forced, half_count, counts)
    starts = jax.random.randint(key_start, (stripes,), 0, 1 << 20) % (stripe_total - counts + 1)
    row_ids = jnp.arange(TILE_ROWS, dtype=jnp.int32)[:, None]
    col_ids = jnp.arange(TILE_COLS, dtype=jnp.int32)[None, :]
    stripe = col_ids // per_row
    run_order = row_ids * per_row + col_ids % per_row - starts[stripe]
    active = (run_order >= 0) & (run_order < counts[stripe])
    levels = jax.random.randint(key_level, (TILE_ROWS, TILE_COLS), 1, 4)
    cost_table = jnp.where(active, levels, 0).astype(jnp.int32)
    owner_table = jnp.where(active, run_order % devices * TILE_SLOTS + run_order // devices, -1).astype(jnp.int32)
    return (cost_table, owner_table)


def draw_tile_cost(key, part):
    return tissue_plan(key)[0]


def draw_tile_owner(key, part):
    return tissue_plan(key)[1]


def label_field(key):
    return (jax.random.randint(jax.random.fold_in(key, 99), (ROWS, COLS), 0, 5) < 2).astype(jnp.int32)


def draw_labels(key, part):
    return label_field(key)


def draw_intensity(key, part):
    label_cells = label_field(key).astype(jnp.float32)
    level_key = jax.random.fold_in(key, 23)
    key_gap, key_sign, key_freq, key_phase, key_amp = jax.random.split(level_key, 5)
    gaps = jax.random.uniform(key_gap, (2,), jnp.float32, 0.05, 0.15)
    signs = jnp.where(jax.random.randint(key_sign, (2,), 0, 2) == 0, -1.0, 1.0).astype(jnp.float32)
    upper_mean = 0.7 + signs[0] * gaps[0]
    lower_mean = 0.3 + signs[1] * gaps[1]
    freqs = jax.random.randint(key_freq, (3, 2), 1, 4).astype(jnp.float32)
    phases = jax.random.uniform(key_phase, (3, 2), jnp.float32, -jnp.pi, jnp.pi)
    amps = jax.random.uniform(key_amp, (3,), jnp.float32, 0.03, 0.05)
    row_pos = jnp.arange(ROWS, dtype=jnp.float32)[:, None] / ROWS
    col_pos = jnp.arange(COLS, dtype=jnp.float32)[None, :] / COLS
    smooth = jnp.zeros((ROWS, COLS), jnp.float32)
    for index in range(3):
        row_wave = jnp.cos(2.0 * jnp.pi * freqs[index, 0] * row_pos + phases[index, 0])
        col_wave = jnp.cos(2.0 * jnp.pi * freqs[index, 1] * col_pos + phases[index, 1])
        smooth = smooth + amps[index] * row_wave * col_wave
    base = lower_mean + (upper_mean - lower_mean) * label_cells + smooth
    noise_key = jax.random.fold_in(key, 17)
    noise = 0.2 * jax.random.normal(noise_key, (ROWS, COLS), jnp.float32)
    return jnp.clip(base + noise, -0.5, 1.5)


def block_scale(stream_key, dims, shards, least, largest):
    factor_of = 1.0
    for axis_at, parts in shards:
        heights = jax.random.uniform(jax.random.fold_in(jax.random.fold_in(stream_key, 6), axis_at), (parts,), jnp.float32, least / len(shards), largest / len(shards))
        factor_of = factor_of * jnp.repeat(jnp.exp(heights), dims[axis_at] // parts).reshape((-1,) + (1,) * (len(dims) - 1 - axis_at))
    return factor_of


def setup_inputs(seed: int = 0) -> dict:
    seeds = jax.random.split(jax.random.key(seed), 6)
    return {
        "intensity": draw_intensity(jax.random.fold_in(seeds[5], 71), 0),
        "edge_weight": jnp.clip(jnp.exp(math.log(2.0) - 2.3025851 * jax.random.uniform(seeds[1], (ROWS, COLS), jnp.float32) ** block_scale(seeds[1], (ROWS, COLS), ((0, 8), (1, 4)), -0.2, 0.2)), 0.2, 2.0),
        "labels": draw_labels(jax.random.fold_in(seeds[5], 71), 0),
        "tile_cost": draw_tile_cost(jax.random.fold_in(seeds[5], 71), 0),
        "tile_owner": draw_tile_owner(jax.random.fold_in(seeds[5], 71), 0),
    }


sigma_step = 0.35
tau_step = 0.35
fidelity = 1.0

def forward_diffs(field):
    grad_down = jnp.concatenate([field[1:] - field[:-1], jnp.zeros_like(field[:1])], axis=0)
    grad_right = jnp.concatenate([field[:, 1:] - field[:, :-1], jnp.zeros_like(field[:, :1])], axis=1)
    return (grad_down, grad_right)

def divergence(flux_down, flux_right):
    above_rim = jnp.concatenate([jnp.zeros_like(flux_down[:1]), flux_down[:-1]], axis=0)
    left_rim = jnp.concatenate([jnp.zeros_like(flux_right[:, :1]), flux_right[:, :-1]], axis=1)
    return flux_down - above_rim + flux_right - left_rim

def expand(table):
    return jnp.repeat(jnp.repeat(table, TILE, axis=0), TILE, axis=1)

def reference(intensity, edge_weight, labels, tile_cost, tile_owner):
    weight_cells = fidelity * expand(tile_cost.astype(jnp.float32))
    tissue = expand(tile_cost > 0)
    relaxed = labels.astype(jnp.float32)
    extrapolated = relaxed
    flux_down = jnp.zeros_like(relaxed)
    flux_right = jnp.zeros_like(relaxed)
    for iteration in range(ITERS_BEFORE + ITERS_AFTER):
        if iteration >= ITERS_BEFORE:
            frozen = jnp.logical_not(tissue)
        else:
            frozen = jnp.zeros(relaxed.shape, bool)
        inside = jnp.sum(relaxed * intensity)
        mass_in = jnp.sum(relaxed)
        outside = jnp.sum((1.0 - relaxed) * intensity)
        mass_out = jnp.sum(1.0 - relaxed)
        region = (intensity - inside / mass_in) ** 2 - (intensity - outside / mass_out) ** 2
        leading = jnp.where(frozen, relaxed, extrapolated)
        grad_down, grad_right = forward_diffs(leading)
        trial_down = flux_down + sigma_step * grad_down
        trial_right = flux_right + sigma_step * grad_right
        length = jnp.sqrt(trial_down * trial_down + trial_right * trial_right)
        shrink = jnp.maximum(1.0, length / edge_weight)
        flux_down = jnp.where(frozen, flux_down, trial_down / shrink)
        flux_right = jnp.where(frozen, flux_right, trial_right / shrink)
        updated = jnp.clip(relaxed + tau_step * (divergence(flux_down, flux_right) - weight_cells * region), 0.0, 1.0)
        updated = jnp.where(frozen, relaxed, updated)
        extrapolated = 2.0 * updated - relaxed
        relaxed = updated
    slot_count = N_ROWS * TILE_SLOTS
    tile_set = relaxed.reshape(TILE_ROWS, TILE, TILE_COLS, TILE).transpose(0, 2, 1, 3)
    stripe = (jnp.arange(TILE_COLS, dtype=jnp.int32) // (BLOCK_COLS // TILE)).astype(jnp.int32)
    stripe_ids = jnp.broadcast_to(stripe[None, :], (TILE_ROWS, TILE_COLS))
    target = jnp.where(tile_owner >= 0, tile_owner, slot_count).astype(jnp.int32)
    result = jnp.zeros((slot_count, N_COLS, TILE, TILE), jnp.float32)
    return result.at[target, stripe_ids].set(tile_set, mode='drop')
```

```python
import functools

import jax
import jax.numpy as jnp
from jax import lax
from jax.experimental import pallas as pl
from jax.experimental.pallas import tpu as pltpu
from jax.sharding import PartitionSpec as P

TILE = 256
ITERS_BEFORE = 2
ITERS_AFTER = 2
ITERS = ITERS_BEFORE + ITERS_AFTER

sigma_step = 0.35
tau_step = 0.35
fidelity = 1.0

SUB = 8
LANES = 128
TOP = 2 * SUB
PRIMAL_BATCH = 4
HALVES = TILE // LANES


def kernel(
    n_rows,
    n_cols,
    cost_ref,
    owner_ref,
    i_hbm,
    e_hbm,
    l_hbm,
    out_ref,
    lab,
    img,
    edge,
    ua,
    ub,
    v,
    gy,
    p1,
    p2,
    moved,
    wmap,
    smap,
    colmask,
    rowmask,
    strip_out,
    strip_in,
    part,
    got,
    pack,
    recv,
    load_sem,
    strip_send,
    strip_recv,
    rim_send,
    rim_recv,
    a_send,
    a_recv,
    t_send,
    t_recv,
):
    height = strip_out.shape[2]
    blocks = lab.shape[0]
    every = blocks + 1
    width = blocks * LANES
    tiles_down, tiles_across = height // TILE, width // TILE
    slots = out_ref.shape[0]
    r = lax.axis_index("rows")
    c = lax.axis_index("cols")
    chunks = height // SUB
    f32 = jnp.float32
    own = pl.ds(TOP, height)

    def load(k, b):
        src = (l_hbm, i_hbm, e_hbm)[k].at[:, pl.ds(b * LANES, LANES)]
        dst = (lab, img, edge)[k].at[b, own, :]
        return pltpu.make_async_copy(src, dst, load_sem.at[k, b])

    ends = [0, blocks - 1]
    inner = list(range(1, blocks - 1))
    order = [(k, b) for b in ends for k in range(3)]
    order += [(k, b) for b in inner for k in range(2)] + [(2, b) for b in inner]
    for k, b in order:
        load(k, b).start()

    def peer(dr, dc):
        return (lax.rem(r + dr, n_rows), lax.rem(c + dc, n_cols))

    others = [(dr, dc) for dr in range(n_rows) for dc in range(n_cols) if dr or dc]
    barrier = pltpu.get_barrier_semaphore()
    for dr, dc in others:
        pl.semaphore_signal(barrier, inc=1, device_id=peer(dr, dc), device_id_type=pl.DeviceIdType.MESH)

    def remote(src, dst, send, arrived, to):
        return pltpu.make_async_remote_copy(
            src_ref=src, dst_ref=dst, send_sem=send, recv_sem=arrived,
            device_id=to, device_id_type=pl.DeviceIdType.MESH,
        )

    lane = lax.broadcasted_iota(jnp.int32, (SUB, LANES), 1)
    sublane = lax.broadcasted_iota(jnp.int32, (SUB, LANES), 0)
    total_bands = n_rows * tiles_down
    total_across = n_cols * tiles_across
    bands = tiles_down + 2
    for band in range(bands):
        tr = jnp.clip(r * tiles_down + band - 1, 0, total_bands - 1)
        for t in range(tiles_across):
            w = cost_ref[tr, c * tiles_across + t].astype(f32)
            for h in range(HALVES):
                wmap[band, t * HALVES + h] = jnp.full((SUB, LANES), w * (tau_step * fidelity), f32)
        right = cost_ref[tr, jnp.clip((c + 1) * tiles_across, 0, total_across - 1)].astype(f32)
        left = cost_ref[tr, jnp.clip(c * tiles_across - 1, 0, total_across - 1)].astype(f32)
        wmap[band, blocks] = (
            jnp.where(lane < LANES // 2, jnp.full((SUB, LANES), right, f32), jnp.full((SUB, LANES), left, f32))
            * (tau_step * fidelity)
        )
    one = jnp.ones((SUB, LANES), f32)
    zero = jnp.zeros((SUB, LANES), f32)
    last_col = (c == n_cols - 1).astype(f32)
    first_col = (c == 0).astype(f32)
    last_row = (r == n_rows - 1).astype(f32)
    first_row = (r == 0).astype(f32)
    edge_lane = (lane == LANES - 1).astype(f32)
    edge_sub = (sublane == SUB - 1).astype(f32)
    colmask[0] = one - edge_lane * last_col
    colmask[1] = one - edge_lane * first_col

    def fill_rows(k, _):
        rowmask[pl.ds(pl.multiple_of(k * SUB, SUB), SUB), :] = one
        return 0

    lax.fori_loop(0, chunks + 4, fill_rows, 0, unroll=4)
    rowmask[SUB:2 * SUB, :] = one - edge_sub * first_row
    rowmask[TOP + height - SUB:TOP + height, :] = one - edge_sub * last_row
    bottom = slice(TOP + height + SUB, TOP + height + 2 * SUB)
    for b in range(every):
        p1[b, 0:SUB, :] = zero
        v[b, bottom, :] = zero

    for b in ends:
        for k in range(3):
            load(k, b).wait()
    for side, b in enumerate(ends):
        take = slice(0, SUB) if side == 0 else slice(LANES - SUB, LANES)
        strip_out[side, 0:SUB, :] = lab[b, TOP:TOP + height, :].astype(f32).T[take]
        strip_out[side, SUB:2 * SUB, :] = img[b, TOP:TOP + height, :].T[take]
        strip_out[side, 2 * SUB:, :] = edge[b, TOP:TOP + height, :].T[take]
    pl.semaphore_wait(barrier, len(others))
    strips = []
    for side, dc in enumerate((n_cols - 1, 1)):
        out, into = strip_out.at[side], strip_in.at[side]
        pieces = (
            (0, pl.ds(0, height), pl.ds(LANES, height)),
            (n_rows - 1, pl.ds(0, LANES), pl.ds(LANES + height, LANES)),
            (1, pl.ds(height - LANES, LANES), pl.ds(0, LANES)),
        )
        for k, (dr, mine, theirs) in enumerate(pieces):
            strips.append(remote(
                out.at[:, mine], into.at[:, theirs],
                strip_send.at[side, k], strip_recv.at[side, k], peer(dr, dc)))
    for strip in strips:
        strip.start()

    def add_sums(acc, fields, images):
        su, si, st = fields[0], images[0], fields[0] * images[0]
        for field, image in zip(fields[1:], images[1:]):
            su, si, st = su + field, si + image, st + field * image
        count = float(len(fields))
        return (acc[0] + st, acc[1] + su, acc[2] + (si - st), acc[3] + (count - su))

    acc = (zero,) * 4
    for b in ends + inner:
        if b in inner:
            load(0, b).wait()
            load(1, b).wait()

        def first(k, acc, b=b):
            base = pl.multiple_of(TOP + k * (PRIMAL_BATCH * SUB), SUB)
            fields, images = [], []
            for j in range(PRIMAL_BATCH):
                rows = pl.ds(pl.multiple_of(base + j * SUB, SUB), SUB)
                field = lab[b, rows, :].astype(f32)
                ua[b, rows, :] = field
                fields.append(field)
                images.append(img[b, rows, :])
            return add_sums(acc, fields, images)

        acc = lax.fori_loop(0, chunks // PRIMAL_BATCH, first, acc, unroll=2)

    def start_sums(it, acc):
        stacked = jnp.concatenate([jnp.sum(x, axis=0, keepdims=True) for x in acc] + [zero[:SUB - 4]], axis=0)
        total = jnp.sum(stacked, axis=1, keepdims=True)
        row = jnp.sum(jnp.where(sublane == lane, total, 0.0), axis=0, keepdims=True)
        part[it] = row
        got[it, len(others):, :] = row
        copies = [
            remote(part.at[it], got.at[it, pl.ds(i, 1)], a_send.at[it, i], a_recv.at[it, i], peer(dr, dc))
            for i, (dr, dc) in enumerate(others)
        ]
        for copy in copies:
            copy.start()
        return copies

    def means(it, copies):
        for copy in copies:
            copy.wait_recv()
        total = jnp.sum(got[it], axis=0, keepdims=True)
        sums = [jnp.broadcast_to(total[:, k:k + 1], (SUB, LANES)) for k in range(4)]
        for copy in copies:
            copy.wait_send()
        return sums[0] / sums[1], sums[2] / sums[3]

    pending = start_sums(0, acc)

    for b in inner:
        load(2, b).wait()
    rims = []
    for k, buf in enumerate((lab, img, edge)):
        part_of = pl.ds(0, blocks)
        rims.append(remote(
            buf.at[part_of, pl.ds(TOP, SUB)], buf.at[part_of, pl.ds(TOP + height, SUB)],
            rim_send.at[2 * k], rim_recv.at[2 * k], peer(n_rows - 1, 0)))
        rims.append(remote(
            buf.at[part_of, pl.ds(TOP + height - SUB, SUB)], buf.at[part_of, pl.ds(TOP - SUB, SUB)],
            rim_send.at[2 * k + 1], rim_recv.at[2 * k + 1], peer(1, 0)))
    for rim in rims:
        rim.start()

    for strip in strips:
        strip.wait()
    middle = jnp.ones((LANES - 2 * SUB, height + 2 * LANES), f32)
    for k, buf in enumerate((ua, img, edge)):
        rows_of = slice(k * SUB, (k + 1) * SUB)
        block = jnp.concatenate([strip_in[0, rows_of, :], middle, strip_in[1, rows_of, :]], axis=0).T
        buf[blocks, TOP - SUB:TOP + height + SUB, :] = block[LANES - SUB:LANES + height + SUB]
    for rim in rims:
        rim.wait()
    for b in range(blocks):
        for rows in (slice(TOP - SUB, TOP), slice(TOP + height, TOP + height + SUB)):
            ua[b, rows, :] = lab[b, rows, :].astype(f32)

    groups = chunks + 2
    batch = next(n for n in (6, 3, 2, 1) if groups % n == 0)
    steps = groups // batch
    per_band = TILE // SUB

    def band_of(g):
        return (g - 2 + per_band) // per_band

    def rows_of_group(g, shift=0):
        base = pl.multiple_of(g * SUB, SUB)
        return pl.ds(base + shift if shift else base, SUB)

    at_last = lane == LANES - 1
    at_first = lane == 0

    def live_of(g):
        return [wmap[band_of(g), b] > 0.0 for b in range(every)]

    def stage_grad(it, new_u, old_u, s):
        for j in range(batch):
            g = 1 + s * batch + j
            rows = rows_of_group(g)
            live = live_of(g) if it == ITERS_BEFORE else None
            fields = []
            for b in range(every):
                field = new_u[b, rows, :]
                if it > 0:
                    ahead = field + (field - old_u[b, rows, :])
                    field = jnp.where(live[b], ahead, field) if live else ahead
                field = field * sigma_step
                v[b, rows, :] = field
                fields.append(field)
            turned = [pltpu.roll(x, LANES - 1, 1) for x in fields]
            for b in range(every):
                grad = jnp.where(at_last, turned[(b + 1) % every], turned[b]) - fields[b]
                if b == blocks - 1:
                    grad = grad * colmask[0]
                if b == blocks:
                    grad = grad * colmask[1]
                gy[b, rows, :] = grad

    def stage_flux(it, s):
        for j in range(batch):
            g = 1 + s * batch + j
            rows = rows_of_group(g)
            mask = rowmask[rows, :]
            live = live_of(g) if it >= ITERS_BEFORE else None
            for b in range(every):
                q1 = (v[b, rows_of_group(g, 1), :] - v[b, rows, :]) * mask
                q2 = gy[b, rows, :]
                if it > 0:
                    old1, old2 = p1[b, rows, :], p2[b, rows, :]
                    q1, q2 = old1 + q1, old2 + q2
                shrink = jnp.minimum(1.0, edge[b, rows, :] * lax.rsqrt(q1 * q1 + q2 * q2))
                q1, q2 = q1 * shrink, q2 * shrink
                if live:
                    q1, q2 = jnp.where(live[b], q1, old1), jnp.where(live[b], q2, old2)
                p1[b, rows, :] = q1
                p2[b, rows, :] = q2

    def stage_div(it, new_u, s):
        for j in range(batch):
            g = 1 + s * batch + j
            rows = rows_of_group(g)
            live = live_of(g) if it >= ITERS_BEFORE else None
            flux = [p2[b, rows, :] for b in range(every)]
            turned = [pltpu.roll(x, 1, 1) for x in flux]
            for b in range(every):
                left = jnp.where(at_first, turned[(b + every - 1) % every], turned[b])
                div = (p1[b, rows, :] - p1[b, rows_of_group(g, -1), :]) + (flux[b] - left)
                old = new_u[b, rows, :]
                ahead = old + div * tau_step
                moved[b, rows, :] = jnp.where(live[b], ahead, old) if live else ahead

    def dual(it, new_u, old_u):
        stage_grad(it, new_u, old_u, 0)
        if steps > 1:
            stage_grad(it, new_u, old_u, 1)

        def step(s, _):
            stage_div(it, new_u, s - 1 + (steps - s) // steps)
            stage_flux(it, s)
            stage_grad(it, new_u, old_u, s + 2 - ((s + 2) // steps) * (s + 3 - steps))
            return 0

        lax.fori_loop(0, steps, step, 0)
        stage_div(it, new_u, steps - 1)

    def settle(moved_at, image, w, middle_mean):
        return jnp.clip(moved_at - w * (image - middle_mean), 0.0, 1.0)

    fields = (ua, ub)
    for it in range(ITERS):
        new_u, old_u = fields[it % 2], fields[(it + 1) % 2]
        dual(it, new_u, old_u)
        c1, c2 = means(it, pending)
        slope = 2.0 * (c2 - c1)
        middle_mean = 0.5 * (c1 + c2)
        if it == ITERS - 1:
            break
        for band in range(bands):
            for b in range(every):
                smap[band, b] = wmap[band, b] * slope

        def update(g, b, w):
            rows = rows_of_group(g)
            image = img[b, rows, :]
            new = settle(moved[b, rows, :], image, w, middle_mean)
            old_u[b, rows, :] = new
            return new, image

        for g in (1, chunks + 2):
            for b in range(every):
                update(g, b, smap[band_of(g), b])

        def step(k, acc):
            g = 2 + k * PRIMAL_BATCH
            band = band_of(g)
            for b in range(every):
                w = smap[band, b]
                pairs = [update(g + j, b, w) for j in range(PRIMAL_BATCH)]
                if b < blocks:
                    acc = add_sums(acc, [x for x, _ in pairs], [y for _, y in pairs])
            return acc

        acc = lax.fori_loop(0, chunks // PRIMAL_BATCH, step, (zero,) * 4)
        pending = start_sums(it + 1, acc)

    own_owner, own_cost = [], []
    for a in range(tiles_down):
        for b in range(tiles_across):
            own_owner.append(owner_ref[r * tiles_down + a, c * tiles_across + b])
            own_cost.append(cost_ref[r * tiles_down + a, c * tiles_across + b])
    step_rows = 4 * SUB

    def fill(dst, k):
        down, across, cost, used = jnp.int32(0), jnp.int32(0), jnp.int32(0), jnp.int32(0)
        for t, o in enumerate(own_owner):
            hit = (o >= k * slots) & (o < (k + 1) * slots)
            down = jnp.where(hit, t // tiles_across, down)
            across = jnp.where(hit, t % tiles_across, across)
            cost = jnp.where(hit, own_cost[t], cost)
            used = jnp.where(hit, 1, used)
        w = slope * (cost.astype(f32) * (tau_step * fidelity))
        scale = used.astype(f32)
        at_down = [jnp.full((SUB, LANES), down, jnp.int32) == a for a in range(tiles_down)]

        def step(j, _):
            for i in range(step_rows // SUB):
                at = pl.multiple_of(j * step_rows + i * SUB, SUB)
                for h in range(HALVES):
                    b = across * HALVES + h
                    ahead, image = zero, zero
                    for a in range(tiles_down):
                        rows = pl.ds(pl.multiple_of(at + (TOP + a * TILE), SUB), SUB)
                        ahead = jnp.where(at_down[a], moved[b, rows, :], ahead)
                        image = jnp.where(at_down[a], img[b, rows, :], image)
                    dst[h, pl.ds(at, SUB), :] = settle(ahead, image, w, middle_mean) * scale
            return 0

        lax.fori_loop(0, TILE // step_rows, step, 0)

    sends = []
    for d in range(1, n_rows):
        to = peer(d, 0)
        fill(pack.at[d - 1], to[0])
        copy = remote(pack.at[d - 1], recv.at[r], t_send.at[d - 1], t_recv.at[d - 1], to)
        copy.start()
        sends.append(copy)
    fill(recv.at[r], r)

    origin = []
    for s in range(slots):
        def look(a, carry):
            source, used = carry
            for b in range(tiles_across):
                hit = owner_ref[a, c * tiles_across + b] == r * slots + s
                source = jnp.where(hit, a // tiles_down, source)
                used = jnp.where(hit, 1, used)
            return source, used
        origin.append(lax.fori_loop(0, total_bands, look, (jnp.int32(0), jnp.int32(0))))

    for copy in sends:
        copy.wait()
    for s in range(slots):
        source, used = origin[s]
        scale = used.astype(f32)

        def step(j, _):
            at = pl.ds(pl.multiple_of(j * step_rows, step_rows), step_rows)
            for h in range(HALVES):
                out_ref[s, 0, at, h * LANES:(h + 1) * LANES] = recv[source, h, at, :] * scale
            return 0

        lax.fori_loop(0, TILE // step_rows, step, 0)


def body(n_rows, n_cols, intensity, edge_weight, labels, tile_cost, tile_owner):
    height, width = intensity.shape
    blocks = width // LANES
    tiles_down, tiles_across = height // TILE, width // TILE
    slots = tiles_down * tiles_across // 2
    others = n_rows * n_cols - 1
    f32 = jnp.float32
    full = pltpu.VMEM((blocks + 1, TOP + height + TOP, LANES), f32)
    dma = pltpu.SemaphoreType.DMA
    anywhere = pl.BlockSpec(memory_space=pl.ANY)
    smem = pl.BlockSpec(memory_space=pltpu.SMEM)
    return pl.pallas_call(
        functools.partial(kernel, n_rows, n_cols),
        out_shape=jax.ShapeDtypeStruct((slots, 1, TILE, TILE), f32),
        in_specs=[smem, smem, anywhere, anywhere, anywhere],
        out_specs=pl.BlockSpec(memory_space=pltpu.VMEM),
        scratch_shapes=[
            pltpu.VMEM((blocks, TOP + height + TOP, LANES), jnp.int32),
            full,
            full,
            full,
            full,
            full,
            full,
            full,
            full,
            full,
            pltpu.VMEM((tiles_down + 2, blocks + 1, SUB, LANES), f32),
            pltpu.VMEM((tiles_down + 2, blocks + 1, SUB, LANES), f32),
            pltpu.VMEM((2, SUB, LANES), f32),
            pltpu.VMEM((TOP + height + TOP, LANES), f32),
            pltpu.VMEM((2, 3 * SUB, height), f32),
            pltpu.VMEM((2, 3 * SUB, height + 2 * LANES), f32),
            pltpu.VMEM((ITERS, 1, LANES), f32),
            pltpu.VMEM((ITERS, others + 1, LANES), f32),
            pltpu.VMEM((n_rows - 1, HALVES, TILE, LANES), f32),
            pltpu.VMEM((n_rows, HALVES, TILE, LANES), f32),
            dma((3, blocks)),
            dma((2, 3)),
            dma((2, 3)),
            dma((6,)),
            dma((6,)),
            dma((ITERS, others)),
            dma((ITERS, others)),
            dma((n_rows - 1,)),
            dma((n_rows - 1,)),
        ],
        compiler_params=pltpu.CompilerParams(
            collective_id=0, has_side_effects=True, vmem_limit_bytes=58 * 1024 * 1024
        ),
    )(tile_cost, tile_owner, intensity, edge_weight, labels)


def solution(mesh):
    return jax.shard_map(
        functools.partial(body, mesh.shape["rows"], mesh.shape["cols"]),
        mesh=mesh,
        in_specs=(P("rows", "cols"), P("rows", "cols"), P("rows", "cols"), P(), P()),
        out_specs=P("rows", "cols", None, None),
        check_vma=False,
    )
```

```python
import functools

import jax
import jax.numpy as jnp
from jax import lax
from jax.experimental import pallas as pl
from jax.experimental.pallas import tpu as pltpu
from jax.sharding import PartitionSpec as P

TILE = 256
ITERS_BEFORE = 2
ITERS_AFTER = 2
ITERS = ITERS_BEFORE + ITERS_AFTER

sigma_step = 0.35
tau_step = 0.35
fidelity = 1.0

SUB = 8
LANES = 128
TOP = 2 * SUB
PRIMAL_BATCH = 4
HALVES = TILE // LANES


def kernel(
    n_rows,
    n_cols,
    cost_ref,
    owner_ref,
    i_hbm,
    e_hbm,
    l_hbm,
    out_ref,
    lab,
    img,
    edge,
    ua,
    ub,
    v,
    gy,
    p1,
    p2,
    moved,
    wmap,
    smap,
    colmask,
    rowmask,
    strip_out,
    strip_in,
    part,
    got,
    pack,
    recv,
    load_sem,
    strip_send,
    strip_recv,
    rim_send,
    rim_recv,
    a_send,
    a_recv,
    t_send,
    t_recv,
):
    height = strip_out.shape[2]
    blocks = lab.shape[0]
    every = blocks + 1
    width = blocks * LANES
    tiles_down, tiles_across = height // TILE, width // TILE
    slots = out_ref.shape[0]
    r = lax.axis_index("rows")
    c = lax.axis_index("cols")
    chunks = height // SUB
    f32 = jnp.float32
    own = pl.ds(TOP, height)

    def load(k, b):
        src = (l_hbm, i_hbm, e_hbm)[k].at[:, pl.ds(b * LANES, LANES)]
        dst = (lab, img, edge)[k].at[b, own, :]
        return pltpu.make_async_copy(src, dst, load_sem.at[k, b])

    ends = [0, blocks - 1]
    inner = list(range(1, blocks - 1))
    order = [(k, b) for b in ends for k in range(3)]
    order += [(k, b) for b in inner for k in range(2)] + [(2, b) for b in inner]
    for k, b in order:
        load(k, b).start()

    def peer(dr, dc):
        return (lax.rem(r + dr, n_rows), lax.rem(c + dc, n_cols))

    others = [(dr, dc) for dr in range(n_rows) for dc in range(n_cols) if dr or dc]
    others.sort(key=lambda at: (-min(at[1], n_cols - at[1]), -min(at[0], n_rows - at[0])))
    barrier = pltpu.get_barrier_semaphore()
    for dr, dc in others:
        pl.semaphore_signal(barrier, inc=1, device_id=peer(dr, dc), device_id_type=pl.DeviceIdType.MESH)

    def remote(src, dst, send, arrived, to):
        return pltpu.make_async_remote_copy(
            src_ref=src, dst_ref=dst, send_sem=send, recv_sem=arrived,
            device_id=to, device_id_type=pl.DeviceIdType.MESH,
        )

    lane = lax.broadcasted_iota(jnp.int32, (SUB, LANES), 1)
    sublane = lax.broadcasted_iota(jnp.int32, (SUB, LANES), 0)
    total_bands = n_rows * tiles_down
    total_across = n_cols * tiles_across
    bands = tiles_down + 2
    for band in range(bands):
        tr = jnp.clip(r * tiles_down + band - 1, 0, total_bands - 1)
        for t in range(tiles_across):
            w = cost_ref[tr, c * tiles_across + t].astype(f32)
            for h in range(HALVES):
                wmap[band, t * HALVES + h] = jnp.full((SUB, LANES), w * (tau_step * fidelity), f32)
        right = cost_ref[tr, jnp.clip((c + 1) * tiles_across, 0, total_across - 1)].astype(f32)
        left = cost_ref[tr, jnp.clip(c * tiles_across - 1, 0, total_across - 1)].astype(f32)
        wmap[band, blocks] = (
            jnp.where(lane < LANES // 2, jnp.full((SUB, LANES), right, f32), jnp.full((SUB, LANES), left, f32))
            * (tau_step * fidelity)
        )
    one = jnp.ones((SUB, LANES), f32)
    zero = jnp.zeros((SUB, LANES), f32)
    last_col = (c == n_cols - 1).astype(f32)
    first_col = (c == 0).astype(f32)
    last_row = (r == n_rows - 1).astype(f32)
    first_row = (r == 0).astype(f32)
    edge_lane = (lane == LANES - 1).astype(f32)
    edge_sub = (sublane == SUB - 1).astype(f32)
    colmask[0] = one - edge_lane * last_col
    colmask[1] = one - edge_lane * first_col

    def fill_rows(k, _):
        rowmask[pl.ds(pl.multiple_of(k * SUB, SUB), SUB), :] = one
        return 0

    lax.fori_loop(0, chunks + 4, fill_rows, 0, unroll=4)
    rowmask[SUB:2 * SUB, :] = one - edge_sub * first_row
    rowmask[TOP + height - SUB:TOP + height, :] = one - edge_sub * last_row
    bottom = slice(TOP + height + SUB, TOP + height + 2 * SUB)
    for b in range(every):
        p1[b, 0:SUB, :] = zero
        v[b, bottom, :] = zero

    for b in ends:
        for k in range(3):
            load(k, b).wait()
    for side, b in enumerate(ends):
        take = slice(0, SUB) if side == 0 else slice(LANES - SUB, LANES)
        strip_out[side, 0:SUB, :] = lab[b, TOP:TOP + height, :].astype(f32).T[take]
        strip_out[side, SUB:2 * SUB, :] = img[b, TOP:TOP + height, :].T[take]
        strip_out[side, 2 * SUB:, :] = edge[b, TOP:TOP + height, :].T[take]
    pl.semaphore_wait(barrier, len(others))
    strips = []
    for side, dc in enumerate((n_cols - 1, 1)):
        out, into = strip_out.at[side], strip_in.at[side]
        pieces = (
            (0, pl.ds(0, height), pl.ds(LANES, height)),
            (n_rows - 1, pl.ds(0, LANES), pl.ds(LANES + height, LANES)),
            (1, pl.ds(height - LANES, LANES), pl.ds(0, LANES)),
        )
        for k, (dr, mine, theirs) in enumerate(pieces):
            strips.append(remote(
                out.at[:, mine], into.at[:, theirs],
                strip_send.at[side, k], strip_recv.at[side, k], peer(dr, dc)))
    for strip in strips:
        strip.start()

    def add_sums(acc, fields, images):
        su, si, st = fields[0], images[0], fields[0] * images[0]
        for field, image in zip(fields[1:], images[1:]):
            su, si, st = su + field, si + image, st + field * image
        count = float(len(fields))
        return (acc[0] + st, acc[1] + su, acc[2] + (si - st), acc[3] + (count - su))

    acc = (zero,) * 4
    for b in ends + inner:
        if b in inner:
            load(0, b).wait()
            load(1, b).wait()

        def first(k, acc, b=b):
            base = pl.multiple_of(TOP + k * (PRIMAL_BATCH * SUB), SUB)
            fields, images = [], []
            for j in range(PRIMAL_BATCH):
                rows = pl.ds(pl.multiple_of(base + j * SUB, SUB), SUB)
                field = lab[b, rows, :].astype(f32)
                ua[b, rows, :] = field
                fields.append(field)
                images.append(img[b, rows, :])
            return add_sums(acc, fields, images)

        acc = lax.fori_loop(0, chunks // PRIMAL_BATCH, first, acc, unroll=2)

    summed = []

    def start_sums(it, acc):
        stacked = jnp.concatenate([jnp.sum(x, axis=0, keepdims=True) for x in acc] + [zero[:SUB - 4]], axis=0)
        total = jnp.sum(stacked, axis=1, keepdims=True)
        row = jnp.sum(jnp.where(sublane == lane, total, 0.0), axis=0, keepdims=True)
        part[it] = row
        got[it, len(others):, :] = row
        copies = [
            remote(part.at[it], got.at[it, pl.ds(i, 1)], a_send.at[it, i], a_recv.at[it, i], peer(dr, dc))
            for i, (dr, dc) in enumerate(others)
        ]
        for copy in copies:
            copy.start()
        summed.extend(copies)
        return copies

    def means(it, copies):
        for copy in copies:
            copy.wait_recv()
        total = jnp.sum(got[it], axis=0, keepdims=True)
        sums = [jnp.broadcast_to(total[:, k:k + 1], (SUB, LANES)) for k in range(4)]
        return sums[0] / sums[1], sums[2] / sums[3]

    pending = start_sums(0, acc)

    for b in inner:
        load(2, b).wait()
    rims = []
    for k, buf in enumerate((lab, img, edge)):
        part_of = pl.ds(0, blocks)
        rims.append(remote(
            buf.at[part_of, pl.ds(TOP, SUB)], buf.at[part_of, pl.ds(TOP + height, SUB)],
            rim_send.at[2 * k], rim_recv.at[2 * k], peer(n_rows - 1, 0)))
        rims.append(remote(
            buf.at[part_of, pl.ds(TOP + height - SUB, SUB)], buf.at[part_of, pl.ds(TOP - SUB, SUB)],
            rim_send.at[2 * k + 1], rim_recv.at[2 * k + 1], peer(1, 0)))
    for rim in rims:
        rim.start()

    for strip in strips:
        strip.wait()
    middle = jnp.ones((LANES - 2 * SUB, height + 2 * LANES), f32)
    for k, buf in enumerate((ua, img, edge)):
        rows_of = slice(k * SUB, (k + 1) * SUB)
        block = jnp.concatenate([strip_in[0, rows_of, :], middle, strip_in[1, rows_of, :]], axis=0).T
        buf[blocks, TOP - SUB:TOP + height + SUB, :] = block[LANES - SUB:LANES + height + SUB]
    for rim in rims:
        rim.wait()
    for b in range(blocks):
        for rows in (slice(TOP - SUB, TOP), slice(TOP + height, TOP + height + SUB)):
            ua[b, rows, :] = lab[b, rows, :].astype(f32)

    groups = chunks + 2
    batch = next(n for n in (6, 3, 2, 1) if groups % n == 0)
    steps = groups // batch
    per_band = TILE // SUB

    def band_of(g):
        return (g - 2 + per_band) // per_band

    def rows_of_group(g, shift=0):
        base = pl.multiple_of(g * SUB, SUB)
        return pl.ds(base + shift if shift else base, SUB)

    at_last = lane == LANES - 1
    at_first = lane == 0

    def live_of(g):
        return [wmap[band_of(g), b] > 0.0 for b in range(every)]

    def stage_grad(it, new_u, old_u, s):
        for j in range(batch):
            g = 1 + s * batch + j
            rows = rows_of_group(g)
            live = live_of(g) if it == ITERS_BEFORE else None
            fields = []
            for b in range(every):
                field = new_u[b, rows, :]
                if it > 0:
                    ahead = field + (field - old_u[b, rows, :])
                    field = jnp.where(live[b], ahead, field) if live else ahead
                field = field * sigma_step
                v[b, rows, :] = field
                fields.append(field)
            turned = [pltpu.roll(x, LANES - 1, 1) for x in fields]
            for b in range(every):
                grad = jnp.where(at_last, turned[(b + 1) % every], turned[b]) - fields[b]
                if b == blocks - 1:
                    grad = grad * colmask[0]
                if b == blocks:
                    grad = grad * colmask[1]
                gy[b, rows, :] = grad

    def stage_flux(it, s):
        for j in range(batch):
            g = 1 + s * batch + j
            rows = rows_of_group(g)
            mask = rowmask[rows, :]
            live = live_of(g) if it >= ITERS_BEFORE else None
            for b in range(every):
                q1 = (v[b, rows_of_group(g, 1), :] - v[b, rows, :]) * mask
                q2 = gy[b, rows, :]
                if it > 0:
                    old1, old2 = p1[b, rows, :], p2[b, rows, :]
                    q1, q2 = old1 + q1, old2 + q2
                shrink = jnp.minimum(1.0, edge[b, rows, :] * lax.rsqrt(q1 * q1 + q2 * q2))
                q1, q2 = q1 * shrink, q2 * shrink
                if live:
                    q1, q2 = jnp.where(live[b], q1, old1), jnp.where(live[b], q2, old2)
                p1[b, rows, :] = q1
                p2[b, rows, :] = q2

    def stage_div(it, new_u, s):
        for j in range(batch):
            g = 1 + s * batch + j
            rows = rows_of_group(g)
            live = live_of(g) if it >= ITERS_BEFORE else None
            flux = [p2[b, rows, :] for b in range(every)]
            turned = [pltpu.roll(x, 1, 1) for x in flux]
            for b in range(every):
                left = jnp.where(at_first, turned[(b + every - 1) % every], turned[b])
                div = (p1[b, rows, :] - p1[b, rows_of_group(g, -1), :]) + (flux[b] - left)
                old = new_u[b, rows, :]
                ahead = old + div * tau_step
                moved[b, rows, :] = jnp.where(live[b], ahead, old) if live else ahead

    def dual(it, new_u, old_u):
        stage_grad(it, new_u, old_u, 0)
        if steps > 1:
            stage_grad(it, new_u, old_u, 1)

        def step(s, _):
            stage_div(it, new_u, s - 1 + (steps - s) // steps)
            stage_flux(it, s)
            stage_grad(it, new_u, old_u, s + 2 - ((s + 2) // steps) * (s + 3 - steps))
            return 0

        lax.fori_loop(0, steps, step, 0)
        stage_div(it, new_u, steps - 1)

    def settle(moved_at, image, w, middle_mean):
        return jnp.clip(moved_at - w * (image - middle_mean), 0.0, 1.0)

    fields = (ua, ub)
    for it in range(ITERS):
        new_u, old_u = fields[it % 2], fields[(it + 1) % 2]
        dual(it, new_u, old_u)
        c1, c2 = means(it, pending)
        slope = 2.0 * (c2 - c1)
        middle_mean = 0.5 * (c1 + c2)
        if it == ITERS - 1:
            break
        for band in range(bands):
            for b in range(every):
                smap[band, b] = wmap[band, b] * slope

        def update(g, b, w):
            rows = rows_of_group(g)
            image = img[b, rows, :]
            new = settle(moved[b, rows, :], image, w, middle_mean)
            old_u[b, rows, :] = new
            return new, image

        for g in (1, chunks + 2):
            for b in range(every):
                update(g, b, smap[band_of(g), b])

        def step(k, acc):
            g = 2 + k * PRIMAL_BATCH
            band = band_of(g)
            for b in range(every):
                w = smap[band, b]
                pairs = [update(g + j, b, w) for j in range(PRIMAL_BATCH)]
                if b < blocks:
                    acc = add_sums(acc, [x for x, _ in pairs], [y for _, y in pairs])
            return acc

        acc = lax.fori_loop(0, chunks // PRIMAL_BATCH, step, (zero,) * 4)
        pending = start_sums(it + 1, acc)

    own_owner, own_cost = [], []
    for a in range(tiles_down):
        for b in range(tiles_across):
            own_owner.append(owner_ref[r * tiles_down + a, c * tiles_across + b])
            own_cost.append(cost_ref[r * tiles_down + a, c * tiles_across + b])
    step_rows = 4 * SUB

    def fill(dst, k):
        down, across, cost, used = jnp.int32(0), jnp.int32(0), jnp.int32(0), jnp.int32(0)
        for t, o in enumerate(own_owner):
            hit = (o >= k * slots) & (o < (k + 1) * slots)
            down = jnp.where(hit, t // tiles_across, down)
            across = jnp.where(hit, t % tiles_across, across)
            cost = jnp.where(hit, own_cost[t], cost)
            used = jnp.where(hit, 1, used)
        w = slope * (cost.astype(f32) * (tau_step * fidelity))
        scale = used.astype(f32)
        at_down = [jnp.full((SUB, LANES), down, jnp.int32) == a for a in range(tiles_down)]

        def step(j, _):
            for i in range(step_rows // SUB):
                at = pl.multiple_of(j * step_rows + i * SUB, SUB)
                for h in range(HALVES):
                    b = across * HALVES + h
                    ahead, image = zero, zero
                    for a in range(tiles_down):
                        rows = pl.ds(pl.multiple_of(at + (TOP + a * TILE), SUB), SUB)
                        ahead = jnp.where(at_down[a], moved[b, rows, :], ahead)
                        image = jnp.where(at_down[a], img[b, rows, :], image)
                    dst[h, pl.ds(at, SUB), :] = settle(ahead, image, w, middle_mean) * scale
            return 0

        lax.fori_loop(0, TILE // step_rows, step, 0)

    sends = []
    for d in range(1, n_rows):
        to = peer(d, 0)
        fill(pack.at[d - 1], to[0])
        copy = remote(pack.at[d - 1], recv.at[r], t_send.at[d - 1], t_recv.at[d - 1], to)
        copy.start()
        sends.append(copy)
    fill(recv.at[r], r)

    origin = []
    for s in range(slots):
        def look(a, carry):
            source, used = carry
            for b in range(tiles_across):
                hit = owner_ref[a, c * tiles_across + b] == r * slots + s
                source = jnp.where(hit, a // tiles_down, source)
                used = jnp.where(hit, 1, used)
            return source, used
        origin.append(lax.fori_loop(0, total_bands, look, (jnp.int32(0), jnp.int32(0))))

    for copy in summed:
        copy.wait_send()
    for copy in sends:
        copy.wait()
    for s in range(slots):
        source, used = origin[s]
        scale = used.astype(f32)

        def step(j, _):
            at = pl.ds(pl.multiple_of(j * step_rows, step_rows), step_rows)
            for h in range(HALVES):
                out_ref[s, 0, at, h * LANES:(h + 1) * LANES] = recv[source, h, at, :] * scale
            return 0

        lax.fori_loop(0, TILE // step_rows, step, 0)


def body(n_rows, n_cols, intensity, edge_weight, labels, tile_cost, tile_owner):
    height, width = intensity.shape
    blocks = width // LANES
    tiles_down, tiles_across = height // TILE, width // TILE
    slots = tiles_down * tiles_across // 2
    others = n_rows * n_cols - 1
    f32 = jnp.float32
    full = pltpu.VMEM((blocks + 1, TOP + height + TOP, LANES), f32)
    dma = pltpu.SemaphoreType.DMA
    anywhere = pl.BlockSpec(memory_space=pl.ANY)
    smem = pl.BlockSpec(memory_space=pltpu.SMEM)
    return pl.pallas_call(
        functools.partial(kernel, n_rows, n_cols),
        out_shape=jax.ShapeDtypeStruct((slots, 1, TILE, TILE), f32),
        in_specs=[smem, smem, anywhere, anywhere, anywhere],
        out_specs=pl.BlockSpec(memory_space=pltpu.VMEM),
        scratch_shapes=[
            pltpu.VMEM((blocks, TOP + height + TOP, LANES), jnp.int32),
            full,
            full,
            full,
            full,
            full,
            full,
            full,
            full,
            full,
            pltpu.VMEM((tiles_down + 2, blocks + 1, SUB, LANES), f32),
            pltpu.VMEM((tiles_down + 2, blocks + 1, SUB, LANES), f32),
            pltpu.VMEM((2, SUB, LANES), f32),
            pltpu.VMEM((TOP + height + TOP, LANES), f32),
            pltpu.VMEM((2, 3 * SUB, height), f32),
            pltpu.VMEM((2, 3 * SUB, height + 2 * LANES), f32),
            pltpu.VMEM((ITERS, 1, LANES), f32),
            pltpu.VMEM((ITERS, others + 1, LANES), f32),
            pltpu.VMEM((n_rows - 1, HALVES, TILE, LANES), f32),
            pltpu.VMEM((n_rows, HALVES, TILE, LANES), f32),
            dma((3, blocks)),
            dma((2, 3)),
            dma((2, 3)),
            dma((6,)),
            dma((6,)),
            dma((ITERS, others)),
            dma((ITERS, others)),
            dma((n_rows - 1,)),
            dma((n_rows - 1,)),
        ],
        compiler_params=pltpu.CompilerParams(
            collective_id=0, has_side_effects=True, vmem_limit_bytes=58 * 1024 * 1024
        ),
    )(tile_cost, tile_owner, intensity, edge_weight, labels)


def solution(mesh):
    return jax.shard_map(
        functools.partial(body, mesh.shape["rows"], mesh.shape["cols"]),
        mesh=mesh,
        in_specs=(P("rows", "cols"), P("rows", "cols"), P("rows", "cols"), P(), P()),
        out_specs=P("rows", "cols", None, None),
        check_vma=False,
    )
```
